32 devices in a mesh: lat: 8 (over z, y), rad: 4 (over x, core).
Axes of the slice: x: 2, y: 2, z: 4, core: 2. Of those that a mesh axis runs over, the one named last changes fastest.
Arguments:
- displacement: float32 [64, 6144], P('rad', 'lat'), may hold values from -6 to 6
- surface_load: float32 [64, 6144], P('rad', 'lat'), may hold values from -6 to 6
- dens_grad: float32 [64, 6144], P('rad', 'lat'), may hold values from 0.5 to 2
- dens_ref: float32 [64], P('rad'), may hold values from 0.5 to 2
- relax_rate: float32 [64, 6144], P('rad', 'lat'), may hold values from 0.02 to 0.2
- basis: bfloat16 [2408, 6144], P(None, 'lat'), may hold values from -0.109375 to 0.109375
- neighbours: int32 [4, 6144], P(None, 'lat'), may hold values from 0 to 767
- green: float32 [49, 64, 64], replicated, may hold values from -2.5 to 2.5
Outputs:
- relaxed: float32 [64, 6144], P('rad', 'lat')
- step_sizes: float32 [3], replicated
The draws below stay inside these ranges and needn't reach their ends.
Inputs may be any that keep to these rules, and one draw needn't show every extreme that they name: `neighbours`: indices of columns inside the same tile of 768 columns.
All inputs are finite; a program needn't handle non-finite values.
Results may differ from the reference program's by a relative error of at most 0.0045.
Values may be sent and summed in bfloat16 or wider, within the bound.
No kernel may reach another device: no remote copies, remote signals or barrier semaphores. Data moves between devices by JAX's collectives and lax.ppermute only.
A program may use at most 64 MiB of HBM per device.

```python
import math
import jax
import jax.numpy as jnp
from jax import lax

DEG = 48
L = 64
C_DEV = 768
ITERS = 3
KH = 2401
KP = 2408
C_TOTAL = 6144


def plant(result, stream_key, low, largest):
    extent = result.shape
    place = [jax.random.randint(jax.random.fold_in(stream_key, axis), (), 0, extent[axis]) for axis in range(len(extent))]
    result = result.at[tuple(place)].set(low)
    longest = extent.index(max(extent))
    place[longest] = (place[longest] + 1) % extent[longest]
    return result.at[tuple(place)].set(largest)


def raised(result, rng, source, target, shards_of, factor):
    def block_of(position):
        return (jnp.arange(result.shape[position]) // (result.shape[position] // shards_of)).reshape((-1,) + (1,) * (result.ndim - 1 - position))

    one_side = jax.random.permutation(rng, shards_of)[block_of(target)]
    second = (block_of(target) + shards_of // 2) % shards_of
    return jnp.where((block_of(source) == one_side) | (block_of(source) == second), factor * result, result)


def shard_levels(rng, dims, shards, smallest, largest):
    loudness, own = 1.0, jax.random.fold_in(rng, 6)
    for position, shards_of in shards:
        heights = jnp.exp(jax.random.uniform(jax.random.fold_in(own, position), (shards_of,), jnp.float32, smallest / len(shards), largest / len(shards)))
        loudness = loudness * jnp.repeat(heights, dims[position] // shards_of).reshape([-1 if axis == position else 1 for axis in range(len(dims))])
    return loudness


def noise(own_key, dims, deviation, reach, shards=(), kind=jnp.bfloat16):
    array = deviation * jax.random.normal(own_key, dims, jnp.float32)
    if shards:
        array = array * shard_levels(own_key, dims, shards, -0.22, 0.18)
    return jnp.clip(array, -reach, reach).astype(kind)


def bell_draw_with(own_key, extent, width, most, cuts, heavy, held_as=jnp.bfloat16):
    values = width * jax.random.normal(own_key, extent, jnp.float32)
    if cuts:
        values = values * shard_levels(own_key, extent, cuts, -0.22, 0.18)
    return jnp.clip(raised(values, jax.random.fold_in(own_key, 3), *heavy), -most, most).astype(held_as)


def setup_inputs(seed: int = 0) -> dict:
    key_of = jax.random.split(jax.random.key(seed), 9)
    return {
        "displacement": noise(key_of[0], (L, C_TOTAL), 1.0, 6.0, ((0, 4), (1, 8)), jnp.float32),
        "surface_load": noise(key_of[1], (L, C_TOTAL), 1.0, 6.0, ((0, 4), (1, 8)), jnp.float32),
        "dens_grad": jnp.clip(jnp.exp(math.log(2.0) - 1.3862944 * jax.random.uniform(key_of[2], (L, C_TOTAL), jnp.float32) ** shard_levels(key_of[2], (L, C_TOTAL), ((0, 4), (1, 8)), -0.2, 0.2)), 0.5, 2.0),
        "dens_ref": jnp.clip(0.5 + 1.5 * jax.random.uniform(key_of[3], (L,), jnp.float32) ** shard_levels(key_of[3], (L,), ((0, 4),), -0.2, 0.2), 0.5, 2.0),
        "relax_rate": jnp.clip(jnp.exp(math.log(0.2) - 2.3025851 * jax.random.uniform(key_of[4], (L, C_TOTAL), jnp.float32) ** shard_levels(key_of[4], (L, C_TOTAL), ((0, 4), (1, 8)), -0.2, 0.2)), 0.02, 0.2),
        "basis": bell_draw_with(key_of[5], (KP, C_TOTAL), C_TOTAL ** -0.5, 0.109375, ((1, 8),), (1, 0, 8, 2.0)),
        "neighbours": plant(jax.random.randint(key_of[6], (4, C_TOTAL), 0, C_DEV), jax.random.fold_in(key_of[6], 1), 0, C_DEV - 1).astype(jnp.int32),
        "green": noise(key_of[7], (DEG + 1, L, L), (max(1, L * KP // (4 * C_TOTAL))) ** -0.5, 2.5, (), jnp.float32),
    }


def radial_step(field):
    padded = jnp.pad(field, ((1, 1), (0, 0)))
    return (padded[2:] - padded[:-2]) * 0.5

def apply_degrees(coefs, green):
    blocks = []
    for degree in range(DEG + 1):
        rows = coefs[degree * degree:(degree + 1) * (degree + 1)]
        blocks.append(lax.dot_general(rows, green[degree], (((1,), (1,)), ((), ())), precision=lax.Precision.HIGHEST, preferred_element_type=jnp.float32))
    blocks.append(jnp.zeros((KP - KH, green.shape[1]), jnp.float32))
    return jnp.concatenate(blocks, axis=0)

def reference(displacement, surface_load, dens_grad, dens_ref, relax_rate, basis, neighbours, green):
    u = displacement
    tile_start = jnp.arange(C_TOTAL, dtype=jnp.int32) // C_DEV * C_DEV
    global_idx = tile_start[None, :] + neighbours
    sizes = []
    for it in range(ITERS):
        rho = (dens_grad * u + dens_ref[:, None] * radial_step(u)).astype(jnp.bfloat16)
        coefs = lax.dot_general(basis, rho, (((1,), (1,)), ((), ())), preferred_element_type=jnp.float32)
        phi = apply_degrees(coefs, green).astype(jnp.bfloat16)
        potential = lax.dot_general(phi, basis, (((0,), (0,)), ((), ())), preferred_element_type=jnp.float32)
        force = radial_step(potential)
        lap = lax.optimization_barrier(jnp.sum(u[:, global_idx], axis=1)) - 4.0 * u
        new = u + relax_rate * (surface_load + force + lap - u)
        sizes.append(jnp.sqrt(jnp.sum((new - u) ** 2) / (L * C_TOTAL)))
        u = new
    return (u, jnp.stack(sizes))
```

```python
import jax
import jax.numpy as jnp
from jax import lax
from jax.experimental import pallas as pl
from jax.experimental.pallas import tpu as pltpu
from jax.sharding import PartitionSpec as P

DEG = 48
L = 64
ITERS = 3
KH = 2401
LANES = 128
HALO = 8

F32, BF16 = jnp.float32, jnp.bfloat16
NT = (((1,), (1,)), ((), ()))
NN = (((1,), (0,)), ((), ()))


def degree_of(k):
    d = 0
    while (d + 1) * (d + 1) <= k:
        d += 1
    return d


def chunks_of(slots, chunk):
    return [(k, min(k + chunk, slots)) for k in range(0, slots, chunk)]


def bf16_parts(x, count):
    parts = []
    for _ in range(count):
        part = x.astype(BF16)
        parts.append(part)
        x = x - part.astype(F32)
    return parts


def build_counts(nb_ref, counts_ref):
    tile = counts_ref.shape[1]
    rows = 32

    def body(b, carry):
        at = pl.multiple_of(b * rows, rows)
        source = lax.broadcasted_iota(jnp.int32, (rows, tile), 0) + at
        total = jnp.zeros((rows, tile), F32)
        for j in range(nb_ref.shape[0]):
            total = total + (source == nb_ref[j : j + 1, :]).astype(F32)
        counts_ref[pl.ds(at, rows), :] = total.astype(BF16)
        return carry

    lax.fori_loop(0, tile // rows, body, 0)


def analyse(u, own, grad_ref, dens_ref, basis_ref, send_ref, squares, chunk):
    rows = u.shape[0]
    above = pltpu.roll(u, rows - 1, 0)
    below = pltpu.roll(u, 1, 0)
    step = (above[:own] - below[:own]) * 0.5
    rho = (grad_ref[...] * u[:own] + dens_ref[...] * step).astype(BF16)
    pieces = chunks_of(basis_ref.shape[0], chunk)
    lane = lax.broadcasted_iota(jnp.int32, (own, LANES), 1)
    row = lax.broadcasted_iota(jnp.int32, (own, LANES), 0)
    if squares is None:
        tail = jnp.zeros((own, LANES), BF16)
    else:
        high, low = [p.astype(F32) for p in bf16_parts(squares, 2)]
        tail = jnp.where(lane == chunk, high, jnp.where(lane == chunk + 1, low, 0.0))
        tail = jnp.where(row == 0, tail, 0.0).astype(BF16)
    for d in range(send_ref.shape[0]):
        send_ref[d] = tail
    for d, (start, end) in enumerate(pieces):
        part = lax.dot_general(rho, basis_ref[start:end, :], NT, preferred_element_type=F32)
        send_ref[d, :, 0 : end - start] = part.astype(BF16)


def advance(recv_ref, u_ref, load_ref, rate_ref, basis_ref, counts_ref, own, chunk):
    u = u_ref[...]
    rows = u.shape[0]
    force = jnp.zeros(u.shape, F32)
    for d, (start, end) in enumerate(chunks_of(basis_ref.shape[0], chunk)):
        force = force + lax.dot_general(
            recv_ref[d][:, 0 : end - start], basis_ref[start:end, :], NN, preferred_element_type=F32
        )
    parts = jnp.concatenate([p.astype(F32) for p in bf16_parts(u, 3)], axis=0).astype(BF16)
    sums = lax.dot_general(parts, counts_ref[...], NN, preferred_element_type=F32)
    lap = sums[:rows] + sums[rows : 2 * rows] + sums[2 * rows :] - 4.0 * u
    new = u + rate_ref[...] * (load_ref[...] + force + lap - u)
    change = (new - u)[:own]
    squares = jnp.sum(jnp.sum(change * change, axis=0, keepdims=True), axis=1, keepdims=True)
    return new, squares


def first_kernel(own, chunk, u0, load0, rate0, halo, grad, dens, basis, nb, u, load, rate, counts, send):
    for i, (block, out) in enumerate(((u0, u), (load0, load), (rate0, rate))):
        row = lax.broadcasted_iota(jnp.int32, (HALO, block.shape[1]), 0)
        edge = jnp.where(row == 0, halo[0, i : i + 1, :], 0.0)
        edge = jnp.where(row == HALO - 1, halo[1, i : i + 1, :], edge)
        out[...] = jnp.concatenate([block[...], edge], axis=0)
    build_counts(nb, counts)
    analyse(u[...], own, grad, dens, basis, send, None, chunk)


def middle_kernel(own, chunk, recv, u, load, rate, grad, dens, basis, counts, u_out, send):
    new, squares = advance(recv, u, load, rate, basis, counts, own, chunk)
    u_out[...] = new
    analyse(new, own, grad, dens, basis, send, squares, chunk)


def last_kernel(own, chunk, recv, u, load, rate, basis, counts, relaxed, send):
    new, squares = advance(recv, u, load, rate, basis, counts, own, chunk)
    relaxed[...] = new[:own]
    send[...] = jnp.broadcast_to(squares.reshape(1, 1, 1), send.shape)


def harmonic_kernel(lats, rads, chunk, degrees, first, recv, green, send, total, phi_ref):
    own = recv.shape[1]
    layers = rads * own
    device = lax.axis_index("lat") * rads + lax.axis_index("rad")
    blocks = []
    for j in range(rads):
        block = recv[j].astype(F32)
        for i in range(1, lats):
            block = block + recv[i * rads + j].astype(F32)
        blocks.append(block)
    coefs = jnp.concatenate(blocks, axis=0)
    lane = lax.broadcasted_iota(jnp.int32, (layers, LANES), 1)
    extra = jnp.where(lane >= chunk, coefs, 0.0)
    squares = jnp.sum(jnp.sum(extra, axis=0, keepdims=True), axis=1, keepdims=True)
    total[...] = jnp.broadcast_to(squares, total.shape)
    every = lax.dot_general(
        green[...], coefs, NN, precision=lax.Precision.HIGHEST, preferred_element_type=F32
    )
    k = lane + device * chunk
    low = first(device)
    phi = jnp.zeros((layers, LANES), F32)
    for n in range(degrees):
        degree = low + n
        mine = (k >= degree * degree) & (k < (degree + 1) * (degree + 1)) & (lane < chunk)
        phi = phi + jnp.where(mine, every[n * layers : (n + 1) * layers], 0.0)
    side = own + HALO
    edge = jnp.zeros((side, LANES), F32)
    phi_ref[0:side, :] = edge
    phi_ref[side : side + layers, :] = phi
    phi_ref[side + layers : side + layers + side, :] = edge
    row = lax.broadcasted_iota(jnp.int32, (side, LANES), 0)
    for j in range(rads):
        at = side + j * own
        here = phi_ref[at + 1 : at + 1 + side, :] - phi_ref[at - 1 : at - 1 + side, :]
        before = phi_ref[at : at + 1, :] - phi_ref[at - 2 : at - 1, :]
        slab = (jnp.where(row == side - 1, before, here) * 0.5).astype(BF16)
        for i in range(lats):
            send[i * rads + j] = slab


def local(displacement, surface_load, dens_grad, dens_ref, relax_rate, basis, neighbours, green):
    own, columns = displacement.shape
    slots = basis.shape[0]
    lats, rads = lax.axis_size("lat"), lax.axis_size("rad")
    devices = lats * rads
    both = ("lat", "rad")
    chunk = -(-slots // devices)
    chunk = -(-chunk // 16) * 16
    rows = own + HALO
    layers = rads * own
    firsts = [min(degree_of(k), DEG) for k in range(0, devices * chunk, chunk)]
    lasts = [min(degree_of(k + chunk - 1), DEG) for k in range(0, devices * chunk, chunk)]
    degrees = max(b - a + 1 for a, b in zip(firsts, lasts))

    def first(device):
        k = device * chunk
        count = jnp.int32(0)
        for d in range(1, DEG + 1):
            count = count + (k >= d * d).astype(jnp.int32)
        return jnp.minimum(count, DEG + 1 - degrees)

    device = lax.axis_index("lat") * rads + lax.axis_index("rad")
    mine = lax.dynamic_slice_in_dim(green, first(device), degrees, 0).reshape(degrees * L, L)

    up = [(i, i + 1) for i in range(rads - 1)]
    down = [(i + 1, i) for i in range(rads - 1)]
    stack = (displacement, surface_load, relax_rate)
    tops = jnp.concatenate([a[own - 1 :] for a in stack], axis=0)
    bottoms = jnp.concatenate([a[:1] for a in stack], axis=0)
    before = lax.ppermute(tops, "rad", up)
    after = lax.ppermute(bottoms, "rad", down)
    halo = jnp.stack([after, before])
    dens = dens_ref[:, None]

    def struct(shape, dtype=F32):
        return jax.ShapeDtypeStruct(shape, dtype)

    field = struct((rows, columns))
    partial = struct((devices, own, LANES), BF16)
    back = struct((devices, rows, LANES), BF16)

    def bound(kernel, *args):
        def body(*refs):
            kernel(*args, *refs)

        return body

    def exchange(x):
        return lax.all_to_all(x, both, 0, 0, tiled=True)

    u, load, rate, counts, send = pl.pallas_call(
        bound(first_kernel, own, chunk),
        out_shape=(field, field, field, struct((columns, columns), BF16), partial),
        name="first",
    )(displacement, surface_load, relax_rate, halo, dens_grad, dens, basis, neighbours)
    totals = []
    for it in range(ITERS):
        recv = exchange(send)
        send, total = pl.pallas_call(
            bound(harmonic_kernel, lats, rads, chunk, degrees, first),
            out_shape=(back, struct((8, LANES))),
            scratch_shapes=[pltpu.VMEM((layers + 2 * rows, LANES), F32)],
            name="harmonic",
        )(recv, mine)
        totals.append(total[0, 0])
        recv = exchange(send)
        if it < ITERS - 1:
            u, send = pl.pallas_call(
                bound(middle_kernel, own, chunk), out_shape=(field, partial), name="middle"
            )(recv, u, load, rate, dens_grad, dens, basis, counts)
        else:
            relaxed, send = pl.pallas_call(
                bound(last_kernel, own, chunk),
                out_shape=(struct((own, columns)), struct((devices, 1, LANES))),
                name="last",
            )(recv, u, load, rate, basis, counts)
    final = jnp.sum(exchange(send)[:, 0, 0])
    sums = jnp.stack(totals[1:] + [final])
    return (relaxed, jnp.sqrt(sums / (layers * columns * lats)))


def solution(mesh):
    placed = (
        P("rad", "lat"),
        P("rad", "lat"),
        P("rad", "lat"),
        P("rad"),
        P("rad", "lat"),
        P(None, "lat"),
        P(None, "lat"),
        P(),
    )
    return jax.shard_map(
        local, mesh=mesh, in_specs=placed, out_specs=(P("rad", "lat"), P()), check_vma=False
    )
```

```python
import jax
import jax.numpy as jnp
from jax import lax
from jax.experimental import pallas as pl
from jax.experimental.pallas import tpu as pltpu
from jax.sharding import PartitionSpec as P

DEG = 48
L = 64
ITERS = 3
LANES = 128
TAIL = 8
VMEM_LIMIT = 16 << 20
GROUP = 4

F32, BF16 = jnp.float32, jnp.bfloat16
NT = (((1,), (1,)), ((), ()))
NN = (((1,), (0,)), ((), ()))


def degree_of(k):
    d = 0
    while (d + 1) * (d + 1) <= k:
        d += 1
    return d


def chunks_of(slots, chunk):
    return [(k, min(k + chunk, slots)) for k in range(0, slots, chunk)]


def bf16_parts(x, count):
    parts = []
    for _ in range(count):
        part = x.astype(BF16)
        parts.append(part)
        x = x - part.astype(F32)
    return parts


def build_counts(nb_ref, counts_ref):
    tile = counts_ref.shape[1]
    rows = 32

    def body(b, carry):
        at = pl.multiple_of(b * rows, rows)
        source = lax.broadcasted_iota(jnp.int32, (rows, tile), 0) + at
        total = jnp.zeros((rows, tile), F32)
        for j in range(nb_ref.shape[0]):
            total = total + (source == nb_ref[j : j + 1, :]).astype(F32)
        counts_ref[pl.ds(at, rows), :] = total.astype(BF16)
        return carry

    lax.fori_loop(0, tile // rows, body, 0)


def column(row_ref, rows):
    square = (rows, rows)
    same = lax.broadcasted_iota(jnp.int32, square, 0) == lax.broadcasted_iota(jnp.int32, square, 1)
    spread = jnp.broadcast_to(row_ref[...], square)
    return jnp.sum(jnp.where(same, spread, 0.0), axis=1, keepdims=True)


def analyse(u, grad_ref, dens_ref, basis_ref, send_ref, squares, chunk, ready=lambda d: None):
    own, columns = u.shape
    row = lax.broadcasted_iota(jnp.int32, u.shape, 0)
    above = jnp.where(row == own - 1, 0.0, pltpu.roll(u, own - 1, 0))
    below = jnp.where(row == 0, 0.0, pltpu.roll(u, 1, 0))
    rho = grad_ref[...] * u + column(dens_ref, own) * ((above - below) * 0.5)
    side = lax.broadcasted_iota(jnp.int32, (TAIL, columns), 0) % 2
    edges = jnp.where(side == 0, u[:1], u[own - 1 :])
    rows = jnp.concatenate([rho, edges], axis=0).astype(BF16)

    lane = lax.broadcasted_iota(jnp.int32, (own, LANES), 1)
    row = lax.broadcasted_iota(jnp.int32, (own, LANES), 0)
    rest = jnp.zeros((own, LANES), F32)
    values = [dens_ref[:, 0:1], dens_ref[:, own - 1 : own]]
    if squares is not None:
        values.append(squares)
    for n, value in enumerate(values):
        for m, part in enumerate(bf16_parts(value, 3)):
            rest = jnp.where((row == 4 + n) & (lane == chunk + m), part.astype(F32), rest)
    room = LANES - chunk
    low = lax.broadcasted_iota(jnp.int32, (TAIL, LANES), 0)
    pieces = chunks_of(basis_ref.shape[0], chunk)
    for d in range(len(pieces), send_ref.shape[0]):
        send_ref[d] = rest.astype(BF16)
    for d, (start, end) in enumerate(pieces):
        ready(d)
        part = lax.dot_general(rows, basis_ref[start:end, :], NT, preferred_element_type=F32)
        if end - start < LANES:
            part = jnp.concatenate(
                [part, jnp.zeros((own + TAIL, LANES - (end - start)), F32)], axis=1
            )
        sides = part[own:]
        moved = pltpu.roll(sides, chunk, 1)
        if chunk > room:
            moved = jnp.where(low < 2, moved, pltpu.roll(sides, chunk - room, 1))
        moved = jnp.where(low < 4, moved, rest[:TAIL])
        moved = jnp.concatenate([moved, rest[TAIL:]], axis=0)
        send_ref[d] = jnp.where(lane < chunk, part[:own], moved).astype(BF16)


def total_of(x):
    return jnp.sum(jnp.sum(x, axis=0, keepdims=True), axis=1, keepdims=True)


def advance(recv_ref, change_ref, u_ref, rate_ref, basis_ref, chunk):
    force = jnp.zeros(u_ref.shape, F32)
    for d, (start, end) in enumerate(chunks_of(basis_ref.shape[0], chunk)):
        force = force + lax.dot_general(
            recv_ref[d][:, 0 : end - start], basis_ref[start:end, :], NN, preferred_element_type=F32
        )
    change = change_ref[...] + rate_ref[...] * force
    return u_ref[...] + change, total_of(change * change)


def lateral(u, load, rate, counts):
    rows = u.shape[0]
    parts = jnp.concatenate(bf16_parts(u, 3), axis=0)
    sums = lax.dot_general(parts, counts[...], NN, preferred_element_type=F32)
    lap = sums[:rows] + sums[rows : 2 * rows] + sums[2 * rows :] - 4.0 * u
    return rate[...] * (load[...] + lap - u)


def first_kernel(chunk, lows, *refs):
    sources, (counts, change, send, sems) = refs[:8], refs[16:]
    targets = refs[8:16]
    u, load, grad, rate, dens, nb, mine, basis = targets
    green = sources[6]
    device = lax.axis_index("lat") * lax.axis_size("rad") + lax.axis_index("rad")
    copies = []
    slots = basis.shape[0]
    for source, target in zip(sources[:6], targets[:6]):
        copies.append((source, target))
    copies.append((green.at[pl.ds(lows(device), mine.shape[0])], mine))
    groups = chunks_of(slots, GROUP * chunk)
    for start, end in groups:
        copies.append((sources[7].at[start:end], basis.at[start:end]))
    order = [5, 0, 2, 4] + list(range(7, len(copies))) + [1, 3, 6]
    copies = [pltpu.make_async_copy(*c, sems.at[n]) for n, c in enumerate(copies)]
    for n in order:
        copies[n].start()
    copies[5].wait()
    build_counts(nb, counts)
    for n in (0, 2, 4):
        copies[n].wait()

    def ready(d):
        if d % GROUP == 0:
            copies[7 + d // GROUP].wait()

    analyse(u[...], grad, dens, basis, send, None, chunk, ready)
    for n in (1, 3, 6):
        copies[n].wait()
    change[...] = lateral(u[...], load, rate, counts)


def middle_kernel(chunk, recv, change, u, load, rate, grad, dens, basis, counts, u_out, send, later):
    new, squares = advance(recv, change, u, rate, basis, chunk)
    u_out[...] = new
    analyse(new, grad, dens, basis, send, squares, chunk)
    later[...] = lateral(new, load, rate, counts)


def last_kernel(chunk, recv, change, u, rate, basis, relaxed, send):
    new, squares = advance(recv, change, u, rate, basis, chunk)
    relaxed[...] = new
    send[...] = jnp.broadcast_to(squares.reshape(1, 1, 1), send.shape)


def harmonic_kernel(lats, rads, chunk, degrees, lows, recv, green, send, total):
    own = recv.shape[1]
    layers = rads * own
    room = LANES - chunk
    device = lax.axis_index("lat") * rads + lax.axis_index("rad")
    blocks, tops, bottoms, squares = [], [], [], 0.0
    low = lax.broadcasted_iota(jnp.int32, (TAIL, LANES), 0)
    at = lax.broadcasted_iota(jnp.int32, (TAIL, LANES), 1)

    def value(tile, n):
        return total_of(jnp.where((low == 4 + n) & (at >= chunk), tile, 0.0))

    for j in range(rads):
        block = recv[j].astype(F32)
        for i in range(1, lats):
            block = block + recv[i * rads + j].astype(F32)
        tile = block[:TAIL]
        sides = pltpu.roll(tile, room, 1)
        if chunk > room:
            other = pltpu.roll(pltpu.roll(tile, TAIL - 2, 0), 2 * room, 1)
            sides = jnp.where(at < room, sides, other)
        blocks.append(block)
        tops.append(sides[0:1])
        bottoms.append(sides[1:2])
        squares = squares + value(tile, 2)
    total[...] = jnp.broadcast_to(squares, total.shape)
    row = lax.broadcasted_iota(jnp.int32, (own, LANES), 0)
    for j in range(rads):
        block, tile = blocks[j], blocks[j][:TAIL]
        if j > 0:
            edge = (value(tile, 0) * (0.5 / lats)) * bottoms[j - 1]
            block = block - jnp.where(row == 0, edge, 0.0)
        if j < rads - 1:
            edge = (value(tile, 1) * (0.5 / lats)) * tops[j + 1]
            block = block + jnp.where(row == own - 1, edge, 0.0)
        blocks[j] = block
    coefs = jnp.concatenate(blocks, axis=0)
    every = lax.dot_general(
        green[...].reshape(degrees * layers, layers), coefs, NN, precision=lax.Precision.HIGHEST, preferred_element_type=F32
    )
    lane = lax.broadcasted_iota(jnp.int32, (layers, LANES), 1)
    row = lax.broadcasted_iota(jnp.int32, (layers, LANES), 0)
    k = lane + device * chunk
    start = lows(device)
    phi = jnp.zeros((layers, LANES), F32)
    for n in range(degrees):
        degree = start + n
        mine = (k >= degree * degree) & (k < (degree + 1) * (degree + 1)) & (lane < chunk)
        phi = jnp.where(mine, every[n * layers : (n + 1) * layers], phi)
    above = jnp.where(row == layers - 1, 0.0, pltpu.roll(phi, layers - 1, 0))
    below = jnp.where(row == 0, 0.0, pltpu.roll(phi, 1, 0))
    step = ((above - below) * 0.5).astype(BF16)
    for j in range(rads):
        for i in range(lats):
            send[i * rads + j] = step[j * own : (j + 1) * own]


def final_kernel(recv, one, two, sizes, *, nodes):
    last = jnp.sum(recv[...], axis=0)[:, 0:1]
    for n, total in enumerate((one[0:1, 0:1], two[0:1, 0:1], last)):
        sizes[n] = jnp.sqrt(total / nodes)[0, 0]


def local(displacement, surface_load, dens_grad, dens_ref, relax_rate, basis, neighbours, green):
    own, columns = displacement.shape
    slots = basis.shape[0]
    lats, rads = lax.axis_size("lat"), lax.axis_size("rad")
    devices = lats * rads
    both = ("lat", "rad")
    chunk = -(-slots // devices)
    chunk = -(-chunk // 16) * 16
    layers = rads * own
    firsts = [min(degree_of(k), DEG) for k in range(0, devices * chunk, chunk)]
    lasts = [min(degree_of(k + chunk - 1), DEG) for k in range(0, devices * chunk, chunk)]
    degrees = max(b - a + 1 for a, b in zip(firsts, lasts))

    def lows(device):
        k = device * chunk
        count = jnp.int32(0)
        for d in range(1, DEG + 1):
            count = count + (k >= d * d).astype(jnp.int32)
        return jnp.minimum(count, DEG + 1 - degrees)

    dens = dens_ref.reshape(1, own)
    field = pltpu.VMEM((own, columns), F32)
    packet = pltpu.VMEM((devices, own, LANES), BF16)

    def call(name, kernel, args, out_shape, **more):
        def body(*refs):
            kernel(*args, *refs)

        return pl.pallas_call(
            body,
            out_shape=out_shape,
            name=name,
            compiler_params=pltpu.CompilerParams(vmem_limit_bytes=VMEM_LIMIT),
            **more,
        )

    def exchange(x):
        return lax.all_to_all(x, both, 0, 0, tiled=True)

    groups = len(chunks_of(slots, GROUP * chunk))
    u, load, grad, rate, dens, _, mine, basis, counts, change, send = call(
        "first",
        first_kernel,
        (chunk, lows),
        (
            field,
            field,
            field,
            field,
            pltpu.VMEM((1, own), F32),
            pltpu.VMEM(neighbours.shape, jnp.int32),
            pltpu.VMEM((degrees, L, L), F32),
            pltpu.VMEM(basis.shape, BF16),
            pltpu.VMEM((columns, columns), BF16),
            field,
            packet,
        ),
        in_specs=[pl.BlockSpec(memory_space=pltpu.HBM)] * 8,
        scratch_shapes=[pltpu.SemaphoreType.DMA((7 + groups,))],
    )(
        *(
            pltpu.with_memory_space_constraint(x, pltpu.HBM)
            for x in (
                displacement, surface_load, dens_grad, relax_rate, dens, neighbours, green, basis
            )
        )
    )
    totals = []
    for it in range(ITERS):
        send, total = call(
            "harmonic",
            harmonic_kernel,
            (lats, rads, chunk, degrees, lows),
            (packet, pltpu.VMEM((8, LANES), F32)),
        )(exchange(send), mine)
        totals.append(total)
        recv = exchange(send)
        if it < ITERS - 1:
            u, send, change = call("middle", middle_kernel, (chunk,), (field, packet, field))(
                recv, change, u, load, rate, grad, dens, basis, counts
            )
        else:
            relaxed, send = call(
                "last",
                last_kernel,
                (chunk,),
                (
                    jax.ShapeDtypeStruct((own, columns), F32),
                    pltpu.VMEM((devices, 1, LANES), F32),
                ),
            )(recv, change, u, rate, basis)
    nodes = layers * columns * lats
    sizes = call(
        "final",
        lambda *refs: final_kernel(*refs, nodes=nodes),
        (),
        jax.ShapeDtypeStruct((ITERS,), F32),
        out_specs=pl.BlockSpec(memory_space=pltpu.SMEM),
    )(exchange(send), totals[1], totals[2])
    return (relaxed, sizes)


def solution(mesh):
    placed = (
        P("rad", "lat"),
        P("rad", "lat"),
        P("rad", "lat"),
        P("rad"),
        P("rad", "lat"),
        P(None, "lat"),
        P(None, "lat"),
        P(),
    )
    return jax.shard_map(
        local, mesh=mesh, in_specs=placed, out_specs=(P("rad", "lat"), P()), check_vma=False
    )
```

```python
import jax
import jax.numpy as jnp
from jax import lax
from jax.experimental import pallas as pl
from jax.experimental.pallas import tpu as pltpu
from jax.sharding import PartitionSpec as P

DEG = 48
L = 64
ITERS = 3
LANES = 128
TILE = 8
QUARTER = 4
VMEM_LIMIT = 16 << 20
GROUP = 16

F32, BF16 = jnp.float32, jnp.bfloat16
NT = (((1,), (1,)), ((), ()))
NN = (((1,), (0,)), ((), ()))


def degree_of(k):
    d = 0
    while (d + 1) * (d + 1) <= k:
        d += 1
    return d


def chunks_of(slots, chunk):
    return [(k, min(k + chunk, slots)) for k in range(0, slots, chunk)]


def bf16_parts(x, count):
    parts = []
    for _ in range(count):
        part = x.astype(BF16)
        parts.append(part)
        x = x - part.astype(F32)
    return parts


def build_counts(nb_ref, counts_ref):
    tile = counts_ref.shape[1]
    rows = 32

    def body(b, carry):
        at = pl.multiple_of(b * rows, rows)
        source = lax.broadcasted_iota(jnp.int32, (rows, tile), 0) + at
        total = jnp.zeros((rows, tile), F32)
        for j in range(nb_ref.shape[0]):
            total = total + (source == nb_ref[j : j + 1, :]).astype(F32)
        counts_ref[pl.ds(at, rows), :] = total.astype(BF16)
        return carry

    lax.fori_loop(0, tile // rows, body, 0)


def column(row_ref, rows):
    square = (rows, rows)
    same = lax.broadcasted_iota(jnp.int32, square, 0) == lax.broadcasted_iota(jnp.int32, square, 1)
    spread = jnp.broadcast_to(row_ref[...], square)
    return jnp.sum(jnp.where(same, spread, 0.0), axis=1, keepdims=True)


def analyse(u, grad_ref, dens_ref, basis_ref, send_ref, squares, chunk, ready=lambda d: None):
    own, columns = u.shape
    row = lax.broadcasted_iota(jnp.int32, u.shape, 0)
    above = jnp.where(row == own - 1, 0.0, pltpu.roll(u, own - 1, 0))
    below = jnp.where(row == 0, 0.0, pltpu.roll(u, 1, 0))
    rho = grad_ref[...] * u + column(dens_ref, own) * ((above - below) * 0.5)
    side = lax.broadcasted_iota(jnp.int32, (TILE, columns), 0) % 2
    edges = jnp.where(side == 0, u[:1], u[own - 1 :])
    third, over = rho[TILE : TILE + QUARTER], rho[TILE + QUARTER :]
    rows = [rho[:TILE], third, third, over, over, edges]
    rows = jnp.concatenate(rows, axis=0).astype(BF16)

    room, spare = spaces(chunk)
    at = lax.broadcasted_iota(jnp.int32, (TILE, LANES), 1)
    low = lax.broadcasted_iota(jnp.int32, (TILE, LANES), 0)
    rest = jnp.zeros((TILE, LANES), F32)
    values = [dens_ref[:, 0:1], dens_ref[:, own - 1 : own]]
    if squares is not None:
        values.append(squares)
    for n, value in enumerate(values):
        for m, part in enumerate(bf16_parts(value, 3)):
            rest = jnp.where((low == QUARTER + n) & (at == spare + m), part.astype(F32), rest)
    pieces = chunks_of(basis_ref.shape[0], chunk)
    for d in range(len(pieces), send_ref.shape[0]):
        store(send_ref, d, rest, jnp.zeros((TILE, LANES), F32))
    for d, (start, end) in enumerate(pieces):
        ready(d)
        part = lax.dot_general(rows, basis_ref[start:end, :], NT, preferred_element_type=F32)
        if end - start < LANES:
            part = jnp.concatenate(
                [part, jnp.zeros((4 * TILE, LANES - (end - start)), F32)], axis=1
            )
        main, more, over, sides = [part[n : n + TILE] for n in range(0, 4 * TILE, TILE)]
        over, sides = [
            jnp.where(low < split, pltpu.roll(x, chunk, 1), behind(x, chunk))
            for x, split in ((over, QUARTER), (sides, 2))
        ]
        over = jnp.where((at >= spare) & (low >= QUARTER), rest, over)
        main = jnp.where(at < chunk, main, over)
        store(send_ref, d, main, jnp.where(at < chunk, more, sides))


def spaces(chunk):
    room = LANES - chunk
    return room, chunk + max(0, chunk - room)


def behind(x, chunk):
    room, _ = spaces(chunk)
    return pltpu.roll(x, chunk - room, 1) if chunk > room else jnp.zeros_like(x)


def store(ref, d, main, more):
    ref[d, 0] = main[:QUARTER].astype(BF16)
    ref[d, 1] = main[QUARTER:].astype(BF16)
    ref[d, 2] = more[:QUARTER].astype(BF16)


def unfolded(one, two, chunk):
    room, _ = spaces(chunk)
    first = pltpu.roll(one, room, 1)
    if chunk <= room:
        return first
    at = lax.broadcasted_iota(jnp.int32, one.shape, 1)
    return jnp.where(at < room, first, pltpu.roll(two, 2 * room, 1))


def total_of(x):
    return jnp.sum(jnp.sum(x, axis=0, keepdims=True), axis=1, keepdims=True)


def advance(recv_ref, change_ref, u_ref, rate_ref, basis_ref, chunk):
    force = jnp.zeros(u_ref.shape, F32)
    for d, (start, end) in enumerate(chunks_of(basis_ref.shape[0], chunk)):
        packet = [recv_ref[d, n].astype(F32) for n in range(3)]
        packet = jnp.concatenate(packet + [unfolded(packet[0], packet[1], chunk)], axis=0)
        force = force + lax.dot_general(
            packet.astype(BF16)[:, 0 : end - start],
            basis_ref[start:end, :],
            NN,
            preferred_element_type=F32,
        )
    change = change_ref[...] + rate_ref[...] * force
    return u_ref[...] + change, total_of(change * change)


def lateral(u, load, rate, counts):
    rows = u.shape[0]
    parts = jnp.concatenate(bf16_parts(u, 3), axis=0)
    sums = lax.dot_general(parts, counts[...], NN, preferred_element_type=F32)
    lap = sums[:rows] + sums[rows : 2 * rows] + sums[2 * rows :] - 4.0 * u
    return rate[...] * (load[...] + lap - u)


def first_kernel(chunk, lows, *refs):
    sources, (counts, change, send, sems) = refs[:8], refs[16:]
    targets = refs[8:16]
    u, load, grad, rate, dens, nb, mine, basis = targets
    green = sources[6]
    device = lax.axis_index("lat") * lax.axis_size("rad") + lax.axis_index("rad")
    copies = []
    slots = basis.shape[0]
    for source, target in zip(sources[:6], targets[:6]):
        copies.append((source, target))
    copies.append((green.at[pl.ds(lows(device), mine.shape[0])], mine))
    groups = chunks_of(slots, GROUP * chunk)
    for start, end in groups:
        copies.append((sources[7].at[start:end], basis.at[start:end]))
    order = [5, 0, 2, 4] + list(range(7, len(copies))) + [1, 3, 6]
    copies = [pltpu.make_async_copy(*c, sems.at[n]) for n, c in enumerate(copies)]
    for n in order:
        copies[n].start()
    copies[5].wait()
    build_counts(nb, counts)
    for n in (0, 2, 4):
        copies[n].wait()

    def ready(d):
        if d % GROUP == 0:
            copies[7 + d // GROUP].wait()

    analyse(u[...], grad, dens, basis, send, None, chunk, ready)
    for n in (1, 3, 6):
        copies[n].wait()
    change[...] = lateral(u[...], load, rate, counts)


def middle_kernel(chunk, recv, change, u, load, rate, grad, dens, basis, counts, u_out, send, later):
    new, squares = advance(recv, change, u, rate, basis, chunk)
    u_out[...] = new
    analyse(new, grad, dens, basis, send, squares, chunk)
    later[...] = lateral(new, load, rate, counts)


def last_kernel(chunk, recv, change, u, rate, basis, relaxed, send):
    new, squares = advance(recv, change, u, rate, basis, chunk)
    relaxed[...] = new
    send[...] = jnp.broadcast_to(squares.reshape(1, 1, 1), send.shape)


def harmonic_kernel(lats, rads, chunk, degrees, lows, recv, green, send, *total):
    own = 4 * QUARTER
    layers = rads * own
    _, spare = spaces(chunk)
    device = lax.axis_index("lat") * rads + lax.axis_index("rad")
    low = lax.broadcasted_iota(jnp.int32, (QUARTER, LANES), 0)
    at = lax.broadcasted_iota(jnp.int32, (QUARTER, LANES), 1)
    packets, tops, bottoms, squares = [], [], [], 0.0

    def value(tile, n):
        return total_of(jnp.where((low == n) & (at >= spare), tile, 0.0))

    for j in range(rads):
        packet = [recv[j, n].astype(F32) for n in range(3)]
        for i in range(1, lats):
            packet = [x + recv[i * rads + j, n].astype(F32) for n, x in enumerate(packet)]
        packets.append(packet)
        sides = [packet[2][n : n + 1] for n in range(4)]
        tops.append(unfolded(sides[0], sides[2], chunk))
        bottoms.append(unfolded(sides[1], sides[3], chunk))
        if total:
            squares = squares + value(packet[1], 2)
    if total:
        total[0][...] = jnp.broadcast_to(squares, total[0].shape)
    row = lax.broadcasted_iota(jnp.int32, (own, LANES), 0)
    blocks = []
    for j, packet in enumerate(packets):
        block = jnp.concatenate(packet + [unfolded(packet[0], packet[1], chunk)], axis=0)
        if j > 0:
            edge = (value(packet[1], 0) * (0.5 / lats)) * bottoms[j - 1]
            block = block - jnp.where(row == 0, edge, 0.0)
        if j < rads - 1:
            edge = (value(packet[1], 1) * (0.5 / lats)) * tops[j + 1]
            block = block + jnp.where(row == own - 1, edge, 0.0)
        blocks.append(block)
    coefs = jnp.concatenate(blocks, axis=0)
    every = lax.dot_general(
        green[...].reshape(degrees * layers, layers), coefs, NN, precision=lax.Precision.HIGHEST, preferred_element_type=F32
    )
    lane = lax.broadcasted_iota(jnp.int32, (layers, LANES), 1)
    row = lax.broadcasted_iota(jnp.int32, (layers, LANES), 0)
    k = lane + device * chunk
    start = lows(device)
    phi = jnp.zeros((layers, LANES), F32)
    for n in range(degrees):
        degree = start + n
        mine = (k >= degree * degree) & (k < (degree + 1) * (degree + 1)) & (lane < chunk)
        phi = jnp.where(mine, every[n * layers : (n + 1) * layers], phi)
    above = jnp.where(row == layers - 1, 0.0, pltpu.roll(phi, layers - 1, 0))
    below = jnp.where(row == 0, 0.0, pltpu.roll(phi, 1, 0))
    step = (above - below) * 0.5
    for j in range(rads):
        parts = [step[n : n + QUARTER] for n in range(j * own, (j + 1) * own, QUARTER)]
        parts[0] = jnp.where(at < chunk, parts[0], pltpu.roll(parts[3], chunk, 1))
        parts[1] = jnp.where(at < chunk, parts[1], behind(parts[3], chunk))
        parts = [x.astype(BF16) for x in parts[:3]]
        for i in range(lats):
            for n, part in enumerate(parts):
                send[i * rads + j, n] = part


def final_kernel(recv, one, two, sizes, *, nodes):
    last = jnp.sum(recv[...], axis=0)[:, 0:1]
    for n, total in enumerate((one[0:1, 0:1], two[0:1, 0:1], last)):
        sizes[n] = jnp.sqrt(total / nodes)[0, 0]


def local(displacement, surface_load, dens_grad, dens_ref, relax_rate, basis, neighbours, green):
    own, columns = displacement.shape
    slots = basis.shape[0]
    lats, rads = lax.axis_size("lat"), lax.axis_size("rad")
    devices = lats * rads
    both = ("lat", "rad")
    chunk = -(-slots // devices)
    chunk = -(-chunk // 16) * 16
    layers = rads * own
    firsts = [min(degree_of(k), DEG) for k in range(0, devices * chunk, chunk)]
    lasts = [min(degree_of(k + chunk - 1), DEG) for k in range(0, devices * chunk, chunk)]
    degrees = max(b - a + 1 for a, b in zip(firsts, lasts))

    def lows(device):
        k = device * chunk
        count = jnp.int32(0)
        for d in range(1, DEG + 1):
            count = count + (k >= d * d).astype(jnp.int32)
        return jnp.minimum(count, DEG + 1 - degrees)

    dens = dens_ref.reshape(1, own)
    field = pltpu.VMEM((own, columns), F32)
    packet = pltpu.VMEM((devices, 3, QUARTER, LANES), BF16)

    def call(name, kernel, args, out_shape, **more):
        def body(*refs):
            kernel(*args, *refs)

        return pl.pallas_call(
            body,
            out_shape=out_shape,
            name=name,
            compiler_params=pltpu.CompilerParams(vmem_limit_bytes=VMEM_LIMIT),
            **more,
        )

    def exchange(x):
        return lax.all_to_all(x, both, 0, 0, tiled=True)

    groups = len(chunks_of(slots, GROUP * chunk))
    u, load, grad, rate, dens, _, mine, basis, counts, change, send = call(
        "first",
        first_kernel,
        (chunk, lows),
        (
            field,
            field,
            field,
            field,
            pltpu.VMEM((1, own), F32),
            pltpu.VMEM(neighbours.shape, jnp.int32),
            pltpu.VMEM((degrees, L, L), F32),
            pltpu.VMEM(basis.shape, BF16),
            pltpu.VMEM((columns, columns), BF16),
            field,
            packet,
        ),
        in_specs=[pl.BlockSpec(memory_space=pltpu.HBM)] * 8,
        scratch_shapes=[pltpu.SemaphoreType.DMA((7 + groups,))],
    )(
        *(
            pltpu.with_memory_space_constraint(x, pltpu.HBM)
            for x in (
                displacement, surface_load, dens_grad, relax_rate, dens, neighbours, green, basis
            )
        )
    )
    totals = []
    for it in range(ITERS):
        wanted = [pltpu.VMEM((8, LANES), F32)] * (it > 0)
        send, *total = call(
            "harmonic",
            harmonic_kernel,
            (lats, rads, chunk, degrees, lows),
            (packet, *wanted),
        )(exchange(send), mine)
        totals.extend(total)
        recv = exchange(send)
        if it < ITERS - 1:
            u, send, change = call("middle", middle_kernel, (chunk,), (field, packet, field))(
                recv, change, u, load, rate, grad, dens, basis, counts
            )
        else:
            relaxed, send = call(
                "last",
                last_kernel,
                (chunk,),
                (
                    jax.ShapeDtypeStruct((own, columns), F32),
                    pltpu.VMEM((devices, 1, LANES), F32),
                ),
            )(recv, change, u, rate, basis)
    nodes = layers * columns * lats
    sizes = call(
        "final",
        lambda *refs: final_kernel(*refs, nodes=nodes),
        (),
        jax.ShapeDtypeStruct((ITERS,), F32),
        out_specs=pl.BlockSpec(memory_space=pltpu.SMEM),
    )(exchange(send), *totals)
    return (relaxed, sizes)


def solution(mesh):
    placed = (
        P("rad", "lat"),
        P("rad", "lat"),
        P("rad", "lat"),
        P("rad"),
        P("rad", "lat"),
        P(None, "lat"),
        P(None, "lat"),
        P(),
    )
    return jax.shard_map(
        local, mesh=mesh, in_specs=placed, out_specs=(P("rad", "lat"), P()), check_vma=False
    )
```

```python
import jax
import jax.numpy as jnp
from jax import lax
from jax.experimental import pallas as pl
from jax.experimental.pallas import tpu as pltpu
from jax.sharding import PartitionSpec as P

DEG = 48
L = 64
ITERS = 3
LANES = 128
TILE = 8
QUARTER = 4
VMEM_LIMIT = 16 << 20
GROUP = 16

F32, BF16 = jnp.float32, jnp.bfloat16
NT = (((1,), (1,)), ((), ()))
NN = (((1,), (0,)), ((), ()))


def degree_of(k):
    d = 0
    while (d + 1) * (d + 1) <= k:
        d += 1
    return d


def chunks_of(slots, chunk):
    return [(k, min(k + chunk, slots)) for k in range(0, slots, chunk)]


def bf16_parts(x, count):
    parts = []
    for _ in range(count):
        part = x.astype(BF16)
        parts.append(part)
        x = x - part.astype(F32)
    return parts


def column(row_ref, rows):
    square = (rows, rows)
    same = lax.broadcasted_iota(jnp.int32, square, 0) == lax.broadcasted_iota(jnp.int32, square, 1)
    spread = jnp.broadcast_to(row_ref[...], square)
    return jnp.sum(jnp.where(same, spread, 0.0), axis=1, keepdims=True)


def analyse(u, grad_ref, dens_ref, basis_ref, send_ref, squares, chunk, ready=lambda d: None):
    own, columns = u.shape
    row = lax.broadcasted_iota(jnp.int32, u.shape, 0)
    above = jnp.where(row == own - 1, 0.0, pltpu.roll(u, own - 1, 0))
    below = jnp.where(row == 0, 0.0, pltpu.roll(u, 1, 0))
    rho = grad_ref[...] * u + column(dens_ref, own) * ((above - below) * 0.5)
    side = lax.broadcasted_iota(jnp.int32, (TILE, columns), 0) % 2
    edges = jnp.where(side == 0, u[:1], u[own - 1 :])
    third, over = rho[TILE : TILE + QUARTER], rho[TILE + QUARTER :]
    rows = [rho[:TILE], third, third, over, over, edges]
    rows = jnp.concatenate(rows, axis=0).astype(BF16)

    room, spare = spaces(chunk)
    at = lax.broadcasted_iota(jnp.int32, (TILE, LANES), 1)
    low = lax.broadcasted_iota(jnp.int32, (TILE, LANES), 0)
    rest = jnp.zeros((TILE, LANES), F32)
    values = [dens_ref[:, 0:1], dens_ref[:, own - 1 : own]]
    if squares is not None:
        values.append(squares)
    for n, value in enumerate(values):
        for m, part in enumerate(bf16_parts(value, 3)):
            rest = jnp.where((low == QUARTER + n) & (at == spare + m), part.astype(F32), rest)
    pieces = chunks_of(basis_ref.shape[0], chunk)
    for d in range(len(pieces), send_ref.shape[0]):
        store(send_ref, d, rest, jnp.zeros((TILE, LANES), F32))
    for d, (start, end) in enumerate(pieces):
        ready(d)
        part = lax.dot_general(rows, basis_ref[start:end, :], NT, preferred_element_type=F32)
        if end - start < LANES:
            part = jnp.concatenate(
                [part, jnp.zeros((4 * TILE, LANES - (end - start)), F32)], axis=1
            )
        main, more, over, sides = [part[n : n + TILE] for n in range(0, 4 * TILE, TILE)]
        over, sides = [
            jnp.where(low < split, pltpu.roll(x, chunk, 1), behind(x, chunk))
            for x, split in ((over, QUARTER), (sides, 2))
        ]
        over = jnp.where((at >= spare) & (low >= QUARTER), rest, over)
        main = jnp.where(at < chunk, main, over)
        store(send_ref, d, main, jnp.where(at < chunk, more, sides))


def spaces(chunk):
    room = LANES - chunk
    return room, chunk + max(0, chunk - room)


def behind(x, chunk):
    room, _ = spaces(chunk)
    return pltpu.roll(x, chunk - room, 1) if chunk > room else jnp.zeros_like(x)


def store(ref, d, main, more):
    ref[d, 0] = main[:QUARTER].astype(BF16)
    ref[d, 1] = main[QUARTER:].astype(BF16)
    ref[d, 2] = more[:QUARTER].astype(BF16)


def unfolded(one, two, chunk):
    room, _ = spaces(chunk)
    first = pltpu.roll(one, room, 1)
    if chunk <= room:
        return first
    at = lax.broadcasted_iota(jnp.int32, one.shape, 1)
    return jnp.where(at < room, first, pltpu.roll(two, 2 * room, 1))


def total_of(x):
    return jnp.sum(jnp.sum(x, axis=0, keepdims=True), axis=1, keepdims=True)


def advance(recv_ref, change_ref, u_ref, rate_ref, basis_ref, chunk):
    force = jnp.zeros(u_ref.shape, F32)
    for d, (start, end) in enumerate(chunks_of(basis_ref.shape[0], chunk)):
        packet = [recv_ref[d, n].astype(F32) for n in range(3)]
        packet = jnp.concatenate(packet + [unfolded(packet[0], packet[1], chunk)], axis=0)
        force = force + lax.dot_general(
            packet.astype(BF16)[:, 0 : end - start],
            basis_ref[start:end, :],
            NN,
            preferred_element_type=F32,
        )
    change = change_ref[...] + rate_ref[...] * force
    return u_ref[...] + change, total_of(change * change)


def lateral(u, load, rate, nb_ref):
    rows, columns = u.shape
    blocks = [u[:, at : at + LANES] for at in range(0, columns, LANES)]
    sums = []
    for at in range(0, columns, LANES):
        total = None
        for j in range(nb_ref.shape[0]):
            index = jnp.broadcast_to(nb_ref[j : j + 1, at : at + LANES], (rows, LANES))
            inner, outer = lax.rem(index, LANES), lax.div(index, LANES)
            value = jnp.take_along_axis(blocks[0], inner, axis=1)
            for n in range(1, len(blocks)):
                picked = jnp.take_along_axis(blocks[n], inner, axis=1)
                value = jnp.where(outer == n, picked, value)
            total = value if total is None else total + value
        sums.append(total)
    lap = jnp.concatenate(sums, axis=1) - 4.0 * u
    return rate[...] * (load[...] + lap - u)


def first_kernel(chunk, lows, *refs):
    sources, (change, send, sems) = refs[:8], refs[16:]
    targets = refs[8:16]
    u, load, grad, rate, dens, nb, mine, basis = targets
    green = sources[6]
    device = lax.axis_index("lat") * lax.axis_size("rad") + lax.axis_index("rad")
    copies = []
    slots = basis.shape[0]
    for source, target in zip(sources[:6], targets[:6]):
        copies.append((source, target))
    copies.append((green.at[pl.ds(lows(device), mine.shape[0])], mine))
    groups = chunks_of(slots, GROUP * chunk)
    for start, end in groups:
        copies.append((sources[7].at[start:end], basis.at[start:end]))
    order = [0, 5, 2, 4, 1, 3] + list(range(7, len(copies))) + [6]
    copies = [pltpu.make_async_copy(*c, sems.at[n]) for n, c in enumerate(copies)]
    for n in order:
        copies[n].start()
    for n in (0, 2, 4, 5, 1, 3):
        copies[n].wait()
    change[...] = lateral(u[...], load, rate, nb)

    def ready(d):
        if d % GROUP == 0:
            copies[7 + d // GROUP].wait()

    analyse(u[...], grad, dens, basis, send, None, chunk, ready)
    copies[6].wait()


def middle_kernel(chunk, recv, change, u, load, rate, grad, dens, basis, nb, u_out, send, later):
    new, squares = advance(recv, change, u, rate, basis, chunk)
    u_out[...] = new
    analyse(new, grad, dens, basis, send, squares, chunk)
    later[...] = lateral(new, load, rate, nb)


def last_kernel(chunk, recv, change, u, rate, basis, relaxed, send):
    new, squares = advance(recv, change, u, rate, basis, chunk)
    relaxed[...] = new
    send[...] = jnp.broadcast_to(squares.reshape(1, 1, 1), send.shape)


def harmonic_kernel(lats, rads, chunk, degrees, lows, recv, green, send, *total):
    own = 4 * QUARTER
    layers = rads * own
    _, spare = spaces(chunk)
    device = lax.axis_index("lat") * rads + lax.axis_index("rad")
    low = lax.broadcasted_iota(jnp.int32, (QUARTER, LANES), 0)
    at = lax.broadcasted_iota(jnp.int32, (QUARTER, LANES), 1)
    packets, tops, bottoms, squares = [], [], [], 0.0

    def value(tile, n):
        return total_of(jnp.where((low == n) & (at >= spare), tile, 0.0))

    for j in range(rads):
        packet = [recv[j, n].astype(F32) for n in range(3)]
        for i in range(1, lats):
            packet = [x + recv[i * rads + j, n].astype(F32) for n, x in enumerate(packet)]
        packets.append(packet)
        sides = [packet[2][n : n + 1] for n in range(4)]
        tops.append(unfolded(sides[0], sides[2], chunk))
        bottoms.append(unfolded(sides[1], sides[3], chunk))
        if total:
            squares = squares + value(packet[1], 2)
    if total:
        total[0][...] = jnp.broadcast_to(squares, total[0].shape)
    row = lax.broadcasted_iota(jnp.int32, (own, LANES), 0)
    blocks = []
    for j, packet in enumerate(packets):
        block = jnp.concatenate(packet + [unfolded(packet[0], packet[1], chunk)], axis=0)
        if j > 0:
            edge = (value(packet[1], 0) * (0.5 / lats)) * bottoms[j - 1]
            block = block - jnp.where(row == 0, edge, 0.0)
        if j < rads - 1:
            edge = (value(packet[1], 1) * (0.5 / lats)) * tops[j + 1]
            block = block + jnp.where(row == own - 1, edge, 0.0)
        blocks.append(block)
    coefs = jnp.concatenate(blocks, axis=0)
    every = lax.dot_general(
        green[...].reshape(degrees * layers, layers), coefs, NN, precision=lax.Precision.HIGHEST, preferred_element_type=F32
    )
    lane = lax.broadcasted_iota(jnp.int32, (layers, LANES), 1)
    row = lax.broadcasted_iota(jnp.int32, (layers, LANES), 0)
    k = lane + device * chunk
    start = lows(device)
    phi = jnp.zeros((layers, LANES), F32)
    for n in range(degrees):
        degree = start + n
        mine = (k >= degree * degree) & (k < (degree + 1) * (degree + 1)) & (lane < chunk)
        phi = jnp.where(mine, every[n * layers : (n + 1) * layers], phi)
    above = jnp.where(row == layers - 1, 0.0, pltpu.roll(phi, layers - 1, 0))
    below = jnp.where(row == 0, 0.0, pltpu.roll(phi, 1, 0))
    step = (above - below) * 0.5
    for j in range(rads):
        parts = [step[n : n + QUARTER] for n in range(j * own, (j + 1) * own, QUARTER)]
        parts[0] = jnp.where(at < chunk, parts[0], pltpu.roll(parts[3], chunk, 1))
        parts[1] = jnp.where(at < chunk, parts[1], behind(parts[3], chunk))
        parts = [x.astype(BF16) for x in parts[:3]]
        for i in range(lats):
            for n, part in enumerate(parts):
                send[i * rads + j, n] = part


def final_kernel(recv, one, two, sizes, *, nodes):
    last = jnp.sum(recv[...], axis=0)[:, 0:1]
    for n, total in enumerate((one[0:1, 0:1], two[0:1, 0:1], last)):
        sizes[n] = jnp.sqrt(total / nodes)[0, 0]


def local(displacement, surface_load, dens_grad, dens_ref, relax_rate, basis, neighbours, green):
    own, columns = displacement.shape
    slots = basis.shape[0]
    lats, rads = lax.axis_size("lat"), lax.axis_size("rad")
    devices = lats * rads
    both = ("lat", "rad")
    chunk = -(-slots // devices)
    chunk = -(-chunk // 16) * 16
    layers = rads * own
    firsts = [min(degree_of(k), DEG) for k in range(0, devices * chunk, chunk)]
    lasts = [min(degree_of(k + chunk - 1), DEG) for k in range(0, devices * chunk, chunk)]
    degrees = max(b - a + 1 for a, b in zip(firsts, lasts))

    def lows(device):
        k = device * chunk
        count = jnp.int32(0)
        for d in range(1, DEG + 1):
            count = count + (k >= d * d).astype(jnp.int32)
        return jnp.minimum(count, DEG + 1 - degrees)

    dens = dens_ref.reshape(1, own)
    field = pltpu.VMEM((own, columns), F32)
    packet = pltpu.VMEM((devices, 3, QUARTER, LANES), BF16)

    def call(name, kernel, args, out_shape, **more):
        def body(*refs):
            kernel(*args, *refs)

        return pl.pallas_call(
            body,
            out_shape=out_shape,
            name=name,
            compiler_params=pltpu.CompilerParams(vmem_limit_bytes=VMEM_LIMIT),
            **more,
        )

    def exchange(x):
        return lax.all_to_all(x, both, 0, 0, tiled=True)

    groups = len(chunks_of(slots, GROUP * chunk))
    u, load, grad, rate, dens, nb, mine, basis, change, send = call(
        "first",
        first_kernel,
        (chunk, lows),
        (
            field,
            field,
            field,
            field,
            pltpu.VMEM((1, own), F32),
            pltpu.VMEM(neighbours.shape, jnp.int32),
            pltpu.VMEM((degrees, L, L), F32),
            pltpu.VMEM(basis.shape, BF16),
            field,
            packet,
        ),
        in_specs=[pl.BlockSpec(memory_space=pltpu.HBM)] * 8,
        scratch_shapes=[pltpu.SemaphoreType.DMA((7 + groups,))],
    )(
        *(
            pltpu.with_memory_space_constraint(x, pltpu.HBM)
            for x in (
                displacement, surface_load, dens_grad, relax_rate, dens, neighbours, green, basis
            )
        )
    )
    totals = []
    for it in range(ITERS):
        wanted = [pltpu.VMEM((8, LANES), F32)] * (it > 0)
        send, *total = call(
            "harmonic",
            harmonic_kernel,
            (lats, rads, chunk, degrees, lows),
            (packet, *wanted),
        )(exchange(send), mine)
        totals.extend(total)
        recv = exchange(send)
        if it < ITERS - 1:
            u, send, change = call("middle", middle_kernel, (chunk,), (field, packet, field))(
                recv, change, u, load, rate, grad, dens, basis, nb
            )
        else:
            relaxed, send = call(
                "last",
                last_kernel,
                (chunk,),
                (
                    jax.ShapeDtypeStruct((own, columns), F32),
                    pltpu.VMEM((devices, 1, LANES), F32),
                ),
            )(recv, change, u, rate, basis)
    nodes = layers * columns * lats
    sizes = call(
        "final",
        lambda *refs: final_kernel(*refs, nodes=nodes),
        (),
        jax.ShapeDtypeStruct((ITERS,), F32),
        out_specs=pl.BlockSpec(memory_space=pltpu.SMEM),
    )(exchange(send), *totals)
    return (relaxed, sizes)


def solution(mesh):
    placed = (
        P("rad", "lat"),
        P("rad", "lat"),
        P("rad", "lat"),
        P("rad"),
        P("rad", "lat"),
        P(None, "lat"),
        P(None, "lat"),
        P(),
    )
    return jax.shard_map(
        local, mesh=mesh, in_specs=placed, out_specs=(P("rad", "lat"), P()), check_vma=False
    )
```

```python
import jax
import jax.numpy as jnp
from jax import lax
from jax.experimental import pallas as pl
from jax.experimental.pallas import tpu as pltpu
from jax.sharding import PartitionSpec as P

DEG = 48
L = 64
ITERS = 3
LANES = 128
TILE = 8
QUARTER = 4
VMEM_LIMIT = 16 << 20
GROUP = 16

F32, BF16 = jnp.float32, jnp.bfloat16
NT = (((1,), (1,)), ((), ()))
NN = (((1,), (0,)), ((), ()))


def degree_of(k):
    d = 0
    while (d + 1) * (d + 1) <= k:
        d += 1
    return d


def chunks_of(slots, chunk):
    return [(k, min(k + chunk, slots)) for k in range(0, slots, chunk)]


def bf16_parts(x, count):
    parts = []
    for _ in range(count):
        part = x.astype(BF16)
        parts.append(part)
        x = x - part.astype(F32)
    return parts


def column(row_ref, rows):
    square = (rows, rows)
    same = lax.broadcasted_iota(jnp.int32, square, 0) == lax.broadcasted_iota(jnp.int32, square, 1)
    spread = jnp.broadcast_to(row_ref[...], square)
    return jnp.sum(jnp.where(same, spread, 0.0), axis=1, keepdims=True)


def analyse(u, grad_ref, dens_ref, basis_ref, send_ref, squares, chunk, ready=lambda d: None):
    own, columns = u.shape
    row = lax.broadcasted_iota(jnp.int32, u.shape, 0)
    above = jnp.where(row == own - 1, 0.0, pltpu.roll(u, own - 1, 0))
    below = jnp.where(row == 0, 0.0, pltpu.roll(u, 1, 0))
    rho = grad_ref[...] * u + column(dens_ref, own) * ((above - below) * 0.5)
    side = lax.broadcasted_iota(jnp.int32, (TILE, columns), 0) % 2
    edges = jnp.where(side == 0, u[:1], u[own - 1 :])
    third, over = rho[TILE : TILE + QUARTER], rho[TILE + QUARTER :]
    rows = [rho[:TILE], third, third, over, over, edges]
    rows = jnp.concatenate(rows, axis=0).astype(BF16)

    room, spare = spaces(chunk)
    at = lax.broadcasted_iota(jnp.int32, (TILE, LANES), 1)
    low = lax.broadcasted_iota(jnp.int32, (TILE, LANES), 0)
    rest = jnp.zeros((TILE, LANES), F32)
    values = [dens_ref[:, 0:1], dens_ref[:, own - 1 : own]]
    if squares is not None:
        values.append(squares)
    for n, value in enumerate(values):
        for m, part in enumerate(bf16_parts(value, 3)):
            rest = jnp.where((low == QUARTER + n) & (at == spare + m), part.astype(F32), rest)
    pieces = chunks_of(basis_ref.shape[0], chunk)
    for d in range(len(pieces), send_ref.shape[0]):
        store(send_ref, d, rest, jnp.zeros((TILE, LANES), F32))
    for d, (start, end) in enumerate(pieces):
        ready(d)
        part = lax.dot_general(rows, basis_ref[start:end, :], NT, preferred_element_type=F32)
        if end - start < LANES:
            part = jnp.concatenate(
                [part, jnp.zeros((4 * TILE, LANES - (end - start)), F32)], axis=1
            )
        main, more, over, sides = [part[n : n + TILE] for n in range(0, 4 * TILE, TILE)]
        over, sides = [
            jnp.where(low < split, pltpu.roll(x, chunk, 1), behind(x, chunk))
            for x, split in ((over, QUARTER), (sides, 2))
        ]
        over = jnp.where((at >= spare) & (low >= QUARTER), rest, over)
        main = jnp.where(at < chunk, main, over)
        store(send_ref, d, main, jnp.where(at < chunk, more, sides))


def spaces(chunk):
    room = LANES - chunk
    return room, chunk + max(0, chunk - room)


def behind(x, chunk):
    room, _ = spaces(chunk)
    return pltpu.roll(x, chunk - room, 1) if chunk > room else jnp.zeros_like(x)


def store(ref, d, main, more):
    ref[d, 0] = main[:QUARTER].astype(BF16)
    ref[d, 1] = main[QUARTER:].astype(BF16)
    ref[d, 2] = more[:QUARTER].astype(BF16)


def unfolded(one, two, chunk):
    room, _ = spaces(chunk)
    first = pltpu.roll(one, room, 1)
    if chunk <= room:
        return first
    at = lax.broadcasted_iota(jnp.int32, one.shape, 1)
    return jnp.where(at < room, first, pltpu.roll(two, 2 * room, 1))


def total_of(x):
    return jnp.sum(jnp.sum(x, axis=0, keepdims=True), axis=1, keepdims=True)


def advance(recv_ref, change_ref, u_ref, rate_ref, basis_ref, chunk):
    force = jnp.zeros(u_ref.shape, F32)
    for d, (start, end) in enumerate(chunks_of(basis_ref.shape[0], chunk)):
        packet = [recv_ref[d, n].astype(F32) for n in range(3)]
        packet = jnp.concatenate(packet + [unfolded(packet[0], packet[1], chunk)], axis=0)
        force = force + lax.dot_general(
            packet.astype(BF16)[:, 0 : end - start],
            basis_ref[start:end, :],
            NN,
            preferred_element_type=F32,
        )
    change = change_ref[...] + rate_ref[...] * force
    return u_ref[...] + change, total_of(change * change)


def lateral(u, load, rate, nb_ref):
    rows, columns = u.shape
    blocks = [u[:, at : at + LANES] for at in range(0, columns, LANES)]
    sums = []
    for at in range(0, columns, LANES):
        total = None
        for j in range(nb_ref.shape[0]):
            index = jnp.broadcast_to(nb_ref[j : j + 1, at : at + LANES], (rows, LANES))
            inner, outer = lax.rem(index, LANES), lax.div(index, LANES)
            value = jnp.take_along_axis(blocks[0], inner, axis=1)
            for n in range(1, len(blocks)):
                picked = jnp.take_along_axis(blocks[n], inner, axis=1)
                value = jnp.where(outer == n, picked, value)
            total = value if total is None else total + value
        sums.append(total)
    lap = jnp.concatenate(sums, axis=1) - 4.0 * u
    return rate[...] * (load[...] + lap - u)


def first_kernel(chunk, lows, *refs):
    sources, (parts, change, send, sems) = refs[:8], refs[16:]
    targets = refs[8:16]
    u, load, grad, rate, dens, nb, mine, basis = targets
    green = sources[6]
    device = lax.axis_index("lat") * lax.axis_size("rad") + lax.axis_index("rad")
    copies = []
    slots = basis.shape[0]
    for source, target in zip(sources[:6], targets[:6]):
        copies.append((source, target))
    copies.append((green.at[pl.ds(lows(device), mine.shape[0])], mine))
    pieces, groups = chunks_of(slots, chunk), chunks_of(slots, GROUP * chunk)
    for start, end in groups:
        copies.append((sources[7].at[start:end], basis.at[start:end]))
    order = [0, 2, 4, 7, 5, 1, 3, 6] + list(range(8, len(copies)))
    copies = [pltpu.make_async_copy(*c, sems.at[n]) for n, c in enumerate(copies)]
    for n in order:
        copies[n].start()
    for n in (0, 2, 4):
        copies[n].wait()

    def ready(d):
        if d % GROUP == 0:
            copies[7 + d // GROUP].wait()
        if d + GROUP >= len(pieces) and d % GROUP == 0:
            for n in (5, 1, 3, 6):
                copies[n].wait()
            change[...] = lateral(u[...], load, rate, nb)
            flat = mine[...].reshape(parts.shape[0], mine.shape[2])
            high, low = [x.astype(F32) for x in bf16_parts(flat, 2)]
            parts[...] = jnp.concatenate([high, low], axis=1).astype(BF16)

    analyse(u[...], grad, dens, basis, send, None, chunk, ready)


def middle_kernel(chunk, recv, change, u, load, rate, grad, dens, basis, nb, u_out, send, later):
    new, squares = advance(recv, change, u, rate, basis, chunk)
    u_out[...] = new
    analyse(new, grad, dens, basis, send, squares, chunk)
    later[...] = lateral(new, load, rate, nb)


def last_kernel(chunk, recv, change, u, rate, basis, relaxed, send):
    new, squares = advance(recv, change, u, rate, basis, chunk)
    relaxed[...] = new
    send[...] = jnp.broadcast_to(squares.reshape(1, 1, 1), send.shape)


def harmonic_kernel(lats, rads, chunk, degrees, lows, recv, green, send, *total):
    own = 4 * QUARTER
    layers = rads * own
    _, spare = spaces(chunk)
    device = lax.axis_index("lat") * rads + lax.axis_index("rad")
    low = lax.broadcasted_iota(jnp.int32, (QUARTER, LANES), 0)
    at = lax.broadcasted_iota(jnp.int32, (QUARTER, LANES), 1)
    packets, tops, bottoms, squares = [], [], [], 0.0

    def value(tile, n):
        return total_of(jnp.where((low == n) & (at >= spare), tile, 0.0))

    for j in range(rads):
        packet = [recv[j, n].astype(F32) for n in range(3)]
        for i in range(1, lats):
            packet = [x + recv[i * rads + j, n].astype(F32) for n, x in enumerate(packet)]
        packets.append(packet)
        sides = [packet[2][n : n + 1] for n in range(4)]
        tops.append(unfolded(sides[0], sides[2], chunk))
        bottoms.append(unfolded(sides[1], sides[3], chunk))
        if total:
            squares = squares + value(packet[1], 2)
    if total:
        total[0][...] = jnp.broadcast_to(squares, total[0].shape)
    row = lax.broadcasted_iota(jnp.int32, (own, LANES), 0)
    blocks = []
    for j, packet in enumerate(packets):
        block = jnp.concatenate(packet + [unfolded(packet[0], packet[1], chunk)], axis=0)
        if j > 0:
            edge = (value(packet[1], 0) * (0.5 / lats)) * bottoms[j - 1]
            block = block - jnp.where(row == 0, edge, 0.0)
        if j < rads - 1:
            edge = (value(packet[1], 1) * (0.5 / lats)) * tops[j + 1]
            block = block + jnp.where(row == own - 1, edge, 0.0)
        blocks.append(block)
    coefs = jnp.concatenate(blocks, axis=0)
    high, low = bf16_parts(coefs, 2)
    halves = [jnp.concatenate([high, x], axis=1) for x in (low, jnp.zeros_like(low))]
    every = lax.dot_general(
        green[...], jnp.concatenate(halves, axis=0), NN, preferred_element_type=F32
    )
    lane = lax.broadcasted_iota(jnp.int32, (layers, LANES), 1)
    row = lax.broadcasted_iota(jnp.int32, (layers, LANES), 0)
    k = lane + device * chunk
    start = lows(device)
    phi = jnp.zeros((layers, LANES), F32)
    for n in range(degrees):
        degree = start + n
        mine = (k >= degree * degree) & (k < (degree + 1) * (degree + 1)) & (lane < chunk)
        rows = every[n * layers : (n + 1) * layers]
        phi = jnp.where(mine, rows[:, :LANES] + rows[:, LANES:], phi)
    above = jnp.where(row == layers - 1, 0.0, pltpu.roll(phi, layers - 1, 0))
    below = jnp.where(row == 0, 0.0, pltpu.roll(phi, 1, 0))
    step = (above - below) * 0.5
    for j in range(rads):
        parts = [step[n : n + QUARTER] for n in range(j * own, (j + 1) * own, QUARTER)]
        parts[0] = jnp.where(at < chunk, parts[0], pltpu.roll(parts[3], chunk, 1))
        parts[1] = jnp.where(at < chunk, parts[1], behind(parts[3], chunk))
        parts = [x.astype(BF16) for x in parts[:3]]
        for i in range(lats):
            for n, part in enumerate(parts):
                send[i * rads + j, n] = part


def final_kernel(recv, one, two, sizes, *, nodes):
    last = jnp.sum(recv[...], axis=0)[:, 0:1]
    for n, total in enumerate((one[0:1, 0:1], two[0:1, 0:1], last)):
        sizes[n] = jnp.sqrt(total / nodes)[0, 0]


def local(displacement, surface_load, dens_grad, dens_ref, relax_rate, basis, neighbours, green):
    own, columns = displacement.shape
    slots = basis.shape[0]
    lats, rads = lax.axis_size("lat"), lax.axis_size("rad")
    devices = lats * rads
    both = ("lat", "rad")
    chunk = -(-slots // devices)
    chunk = -(-chunk // 16) * 16
    layers = rads * own
    firsts = [min(degree_of(k), DEG) for k in range(0, devices * chunk, chunk)]
    lasts = [min(degree_of(k + chunk - 1), DEG) for k in range(0, devices * chunk, chunk)]
    degrees = max(b - a + 1 for a, b in zip(firsts, lasts))

    def lows(device):
        k = device * chunk
        count = jnp.int32(0)
        for d in range(1, DEG + 1):
            count = count + (k >= d * d).astype(jnp.int32)
        return jnp.minimum(count, DEG + 1 - degrees)

    dens = dens_ref.reshape(1, own)
    field = pltpu.VMEM((own, columns), F32)
    packet = pltpu.VMEM((devices, 3, QUARTER, LANES), BF16)

    def call(name, kernel, args, out_shape, **more):
        def body(*refs):
            kernel(*args, *refs)

        return pl.pallas_call(
            body,
            out_shape=out_shape,
            name=name,
            compiler_params=pltpu.CompilerParams(vmem_limit_bytes=VMEM_LIMIT),
            **more,
        )

    def exchange(x):
        return lax.all_to_all(x, both, 0, 0, tiled=True)

    groups = len(chunks_of(slots, GROUP * chunk))
    u, load, grad, rate, dens, nb, _, basis, mine, change, send = call(
        "first",
        first_kernel,
        (chunk, lows),
        (
            field,
            field,
            field,
            field,
            pltpu.VMEM((1, own), F32),
            pltpu.VMEM(neighbours.shape, jnp.int32),
            pltpu.VMEM((degrees, L, L), F32),
            pltpu.VMEM(basis.shape, BF16),
            pltpu.VMEM((degrees * L, 2 * L), BF16),
            field,
            packet,
        ),
        in_specs=[pl.BlockSpec(memory_space=pltpu.HBM)] * 8,
        scratch_shapes=[pltpu.SemaphoreType.DMA((7 + groups,))],
    )(
        *(
            pltpu.with_memory_space_constraint(x, pltpu.HBM)
            for x in (
                displacement, surface_load, dens_grad, relax_rate, dens, neighbours, green, basis
            )
        )
    )
    totals = []
    for it in range(ITERS):
        wanted = [pltpu.VMEM((8, LANES), F32)] * (it > 0)
        send, *total = call(
            "harmonic",
            harmonic_kernel,
            (lats, rads, chunk, degrees, lows),
            (packet, *wanted),
        )(exchange(send), mine)
        totals.extend(total)
        recv = exchange(send)
        if it < ITERS - 1:
            u, send, change = call("middle", middle_kernel, (chunk,), (field, packet, field))(
                recv, change, u, load, rate, grad, dens, basis, nb
            )
        else:
            relaxed, send = call(
                "last",
                last_kernel,
                (chunk,),
                (
                    jax.ShapeDtypeStruct((own, columns), F32),
                    pltpu.VMEM((devices, 1, LANES), F32),
                ),
            )(recv, change, u, rate, basis)
    nodes = layers * columns * lats
    sizes = call(
        "final",
        lambda *refs: final_kernel(*refs, nodes=nodes),
        (),
        jax.ShapeDtypeStruct((ITERS,), F32),
        out_specs=pl.BlockSpec(memory_space=pltpu.SMEM),
    )(exchange(send), *totals)
    return (relaxed, sizes)


def solution(mesh):
    placed = (
        P("rad", "lat"),
        P("rad", "lat"),
        P("rad", "lat"),
        P("rad"),
        P("rad", "lat"),
        P(None, "lat"),
        P(None, "lat"),
        P(),
    )
    return jax.shard_map(
        local, mesh=mesh, in_specs=placed, out_specs=(P("rad", "lat"), P()), check_vma=False
    )
```
